32 devices in a mesh: batch: 1 (over z), row: 4 (over y), col: 8 (over x, core).
Axes of the slice: x: 4, y: 4, z: 1, core: 2. Of those that a mesh axis runs over, the one named last changes fastest.
The devices are a block of a 4x4x8 slice.
Arguments:
- a_mat: bfloat16 [4096, 65536], P(('batch', 'row'), 'col')
Outputs:
- output: bfloat16 [4096, 4096], P(('batch', 'row'), 'col')
All inputs are finite; a program needn't handle non-finite values.
Results may differ from the reference program's by a relative error of at most 0.001.
Values are sent between devices in bfloat16 or wider.
A program may use at most 768 MiB of HBM per device.

```python
import jax
import jax.numpy as jnp
from jax import lax

N = 4096
BLOCK = 256
M_COLS = 65536
ROW_GROUPS = 4
COL_GROUPS = 8


def setup_inputs(seed: int = 0, part: int = 0) -> dict:
    base_key = jax.random.fold_in(jax.random.key(seed), part)
    values = jax.random.normal(base_key, (N, M_COLS), jnp.float32) * (M_COLS ** -0.25)
    return {"a_mat": values.astype(jnp.bfloat16)}


def global_index(size, groups):
    stored = jnp.arange(size)
    per_group = size // groups
    group_id = stored // per_group
    within = stored % per_group
    return ((within // BLOCK) * groups + group_id) * BLOCK + within % BLOCK


def reference(a_mat):
    blocks = N // BLOCK
    natural = a_mat.reshape(ROW_GROUPS, blocks // ROW_GROUPS, BLOCK, M_COLS).transpose(1, 0, 2, 3)
    col_order = natural.reshape(blocks // COL_GROUPS, COL_GROUPS, BLOCK, M_COLS).transpose(1, 0, 2, 3).reshape(N, M_COLS)
    col_trans = col_order.T
    row_index = global_index(N, ROW_GROUPS).reshape(blocks, BLOCK)
    col_index = global_index(N, COL_GROUPS)

    def one_block(block_item):
        row_blk, idx_blk = block_item
        product = jnp.dot(row_blk, col_trans, preferred_element_type=jnp.float32)
        return jnp.where(idx_blk[:, None] >= col_index[None, :], product, 0.0).astype(jnp.bfloat16)

    result = lax.map(one_block, (a_mat.reshape(blocks, BLOCK, M_COLS), row_index))
    return result.reshape(N, N)
```

```python
import functools

import jax
import jax.numpy as jnp
from jax import lax
from jax.experimental import pallas as pl
from jax.experimental.pallas import tpu as pltpu
from jax.sharding import PartitionSpec as P

BLOCK = 256
HALF = BLOCK // 2
QUART = BLOCK // 4
MESH = pl.DeviceIdType.MESH
F32 = jnp.float32


def kernel(rows, cols, a_ref, c_ref, relay, xin, part, xmid, xdst, red, ymid, ydst,
           d_s, d_r, r_s, r_r, f_s, f_r, loc_s, core_s, core_r,
           xm_s, xm_r, xo_s, xo_r, xa_s, xa_r, ym_s, ym_r, yo_s, yo_r, ya_s, ya_r, credit):
    chips = cols // 2
    y = lax.axis_index("row")
    pos = lax.axis_index("col")
    x, core = lax.div(pos, 2), lax.rem(pos, 2)
    local_rows, m_local = a_ref.shape
    width = m_local // rows
    half_w = width // 2
    steps = local_rows // HALF
    ents = xdst.shape[2]

    def yy(o):
        return lax.rem(y + o, rows)

    def xx(o):
        return lax.rem(x + o, chips)

    up, down = {"row": yy(1)}, {"row": yy(rows - 1)}
    right, left = {"col": 2 * xx(1) + core}, {"col": 2 * xx(chips - 1) + core}
    twin = {"col": 2 * x + 1 - core}
    ydev, xdev = (up, down), (right, left)

    def remote(src, dst, s, r, dev):
        return pltpu.make_async_remote_copy(
            src_ref=src, dst_ref=dst, send_sem=s, recv_sem=r, device_id=dev, device_id_type=MESH)

    def arrived(dst, s, r):
        remote(dst, dst, s, r, twin).wait_recv()

    def left_us(src, s, r):
        remote(src, src, s, r, twin).wait_send()

    barrier = pltpu.get_barrier_semaphore()
    for dev in (up, down, right, left, twin):
        pl.semaphore_signal(barrier, inc=1, device_id=dev, device_id_type=MESH)
    pl.semaphore_wait(barrier, 5)

    def a_piece(h, owner, off, size):
        return a_ref.at[pl.ds(pl.multiple_of(h * HALF, HALF), HALF),
                        pl.ds(pl.multiple_of(owner * width + off, 128), size)]

    def x_piece(h, group, off, size):
        return xin.at[lax.div(h, 2), group, pl.ds(pl.multiple_of(lax.rem(h, 2) * HALF, HALF), HALF), pl.ds(off, size)]

    def direct(h, d):
        return remote(a_piece(h, yy(1 if d == 0 else rows - 1), 0, width), x_piece(h, y, 0, width),
                      d_s.at[d, h], d_r.at[d, h], ydev[d])

    def relay_out(h, d):
        return remote(a_piece(h, yy(2), d * half_w, half_w), relay.at[d, h], r_s.at[d, h], r_r.at[d, h], ydev[d])

    def forward(h, d):
        return remote(relay.at[d, h], x_piece(h, yy(rows - 1 if d == 0 else 1), d * half_w, half_w),
                      f_s.at[d, h], f_r.at[d, h], ydev[d])

    def own(h):
        return pltpu.make_async_copy(a_piece(h, y, 0, width), x_piece(h, y, 0, width), loc_s.at[h])

    def twin_rows(h, off):
        half = pl.ds(pl.multiple_of(lax.rem(h, 2) * HALF, HALF), HALF)
        return xin.at[lax.div(h, 2), :, half, pl.ds(off, width)]

    def to_twin(h):
        return remote(twin_rows(h, 0), twin_rows(h, width), core_s.at[h], core_r.at[h], twin)

    def both(f, h):
        for d in range(2):
            f(h, d).start()

    def pass_on(h):
        for d in range(2):
            arrived(relay.at[d, h], r_s.at[d, h], r_r.at[d, h])
        both(forward, h)

    def have(h):
        own(h).wait()
        for d in range(2):
            arrived(x_piece(h, yy(rows - 1 if d == 0 else 1), 0, width), d_s.at[d, h], d_r.at[d, h])
            arrived(x_piece(h, yy(2), d * half_w, half_w), f_s.at[d, h], f_r.at[d, h])

    def split(t):
        w, kind = lax.div(t, 3), lax.rem(t, 3)
        return w, kind, lax.div(kind, 2)

    def place(t, e):
        w, kind, own_cols = split(t)
        return 2 * w + (1 - own_cols) * kind + own_cols * e, (1 - own_cols) * e + own_cols * lax.div(2 * w, chips)

    def column(t, o, e):
        return chips * place(t, e)[1] + xx(o)

    def low(t, o, e):
        w, _, own_cols = split(t)
        m = column(t, o, e)
        return ((own_cols == 0) & (m < 2 * w)) | ((own_cols == 1) & (m == 2 * w))

    def high(t, o, e):
        w, _, own_cols = split(t)
        m = column(t, o, e)
        return ((own_cols == 0) & (m < 2 * w)) | ((own_cols == 1) & (lax.div(m, 2) == w))

    A, B = pl.ds(0, 2), pl.ds(2, 2)

    def x_mid(t, e, d):
        sl = lax.rem(t, 2)
        return remote(part.at[sl, 1, e, (A, B)[d]], xmid.at[sl, d, e],
                      xm_s.at[d, sl, e], xm_r.at[d, sl, e], xdev[d])

    def x_own(t, e, d):
        sl, half = lax.rem(t, 2), (B, A)[d]
        return remote(part.at[sl, 2 * d, e, half], xdst.at[sl, d, e, half],
                      xo_s.at[d, sl, e], xo_r.at[d, sl, e], xdev[d])

    def x_acc(t, e, d):
        sl, half = lax.rem(t, 2), (A, B)[d]
        return remote(part.at[sl, 2 * d, e, half], xdst.at[sl, d, e, half],
                      xa_s.at[d, sl, e], xa_r.at[d, sl, e], xdev[d])

    def compute(t, o):
        w, sl = lax.div(t, 3), lax.rem(t, 2)

        def one(e, _):
            @pl.when(high(t, o, e))
            def _():
                h, cb = place(t, e)
                j = 2 * column(t, o, e) + core
                sub = pl.ds(pl.multiple_of(lax.rem(h, 2) * HALF, HALF), HALF)
                lhs = xin[w, :, sub, :].reshape(rows * HALF, 2 * width)
                rhs = xin[lax.div(j, rows), lax.rem(j, rows)]
                val = lax.dot_general(lhs, rhs, (((1,), (1,)), ((), ())), preferred_element_type=F32)
                val = val.reshape(rows, HALF, BLOCK)
                if o == 0:
                    red[h, cb] = val
                else:
                    part[sl, o - 1, e] = val
            return 0

        lax.fori_loop(0, ents, one, 0)

    def x_send_mid(t):
        for e in range(ents):
            @pl.when(low(t, 2, e))
            def _():
                x_mid(t, e, 0).start()

            @pl.when(high(t, 2, e))
            def _():
                x_mid(t, e, 1).start()

    def x_send_own(t, d):
        for e in range(ents):
            @pl.when(high(t, 1, e) if d == 0 else low(t, chips - 1, e))
            def _():
                x_own(t, e, d).start()

    def x_pass_on(t):
        sl = lax.rem(t, 2)
        for e in range(ents):
            @pl.when(low(t, 1, e))
            def _():
                arrived(xmid.at[sl, 0, e], xm_s.at[0, sl, e], xm_r.at[0, sl, e])
                part[sl, 0, e, A] += xmid[sl, 0, e]
                x_acc(t, e, 0).start()

            @pl.when(high(t, chips - 1, e))
            def _():
                arrived(xmid.at[sl, 1, e], xm_s.at[1, sl, e], xm_r.at[1, sl, e])
                part[sl, 2, e, B] += xmid[sl, 1, e]
                x_acc(t, e, 1).start()

    def x_finish(t):
        sl = lax.rem(t, 2)
        for e in range(ents):
            h, cb = place(t, e)

            @pl.when(low(t, 0, e))
            def _():
                arrived(xdst.at[sl, 0, e, A], xa_s.at[0, sl, e], xa_r.at[0, sl, e])
                arrived(xdst.at[sl, 1, e, A], xo_s.at[1, sl, e], xo_r.at[1, sl, e])
                red[h, cb, A] = red[h, cb, A] + xdst[sl, 0, e, A] + xdst[sl, 1, e, A]

            @pl.when(high(t, 0, e))
            def _():
                arrived(xdst.at[sl, 0, e, B], xo_s.at[0, sl, e], xo_r.at[0, sl, e])
                arrived(xdst.at[sl, 1, e, B], xa_s.at[1, sl, e], xa_r.at[1, sl, e])
                red[h, cb, B] = red[h, cb, B] + xdst[sl, 0, e, B] + xdst[sl, 1, e, B]

    def x_sent(t):
        sl = lax.rem(t, 2)
        for e in range(ents):
            for o, d, half, s, r, test in (
                    (2, 0, A, xm_s, xm_r, low), (2, 1, B, xm_s, xm_r, high),
                    (1, 0, B, xo_s, xo_r, high), (chips - 1, 1, A, xo_s, xo_r, low),
                    (1, 0, A, xa_s, xa_r, low), (chips - 1, 1, B, xa_s, xa_r, high)):
                @pl.when(test(t, o, e))
                def _():
                    left_us(part.at[sl, o - 1, e, half], s.at[d, sl, e], r.at[d, sl, e])

    def give_credit():
        pl.semaphore_signal(credit.at[0], inc=1, device_id=left, device_id_type=MESH)
        pl.semaphore_signal(credit.at[1], inc=1, device_id=right, device_id_type=MESH)

    def take_credit():
        pl.semaphore_wait(credit.at[0], 1)
        pl.semaphore_wait(credit.at[1], 1)

    T, U = pl.ds(0, QUART), pl.ds(QUART, QUART)

    def exists(t, o, e):
        w, _, own_cols = split(t)
        m = column(t, 0, e)
        return ((own_cols == 0) & (m < 2 * w)) | (
            (own_cols == 1) & (lax.div(m, 2) == w) & (rows * w + yy(o) >= 2 * m + core))

    def y_mid(h, cb, d):
        return remote(red.at[h, cb, yy(2), (T, U)[d]], ymid.at[h, d, cb],
                      ym_s.at[d, h, cb], ym_r.at[d, h, cb], ydev[d])

    def y_own(h, cb, d):
        half = (U, T)[d]
        return remote(red.at[h, cb, yy((1, rows - 1)[d]), half], ydst.at[h, d, cb, half],
                      yo_s.at[d, h, cb], yo_r.at[d, h, cb], ydev[d])

    def y_acc(h, cb, d):
        half = (T, U)[d]
        return remote(red.at[h, cb, yy((1, rows - 1)[d]), half], ydst.at[h, d, cb, half],
                      ya_s.at[d, h, cb], ya_r.at[d, h, cb], ydev[d])

    def y_send(t):
        for e in range(ents):
            h, cb = place(t, e)

            @pl.when(exists(t, 2, e))
            def _():
                for d in range(2):
                    y_mid(h, cb, d).start()
        for e in range(ents):
            h, cb = place(t, e)
            for d in range(2):
                @pl.when(exists(t, (1, rows - 1)[d], e))
                def _():
                    y_own(h, cb, d).start()

    def y_pass_on(t):
        for e in range(ents):
            h, cb = place(t, e)
            for d in range(2):
                o, half = (1, rows - 1)[d], (T, U)[d]

                @pl.when(exists(t, o, e))
                def _():
                    arrived(ymid.at[h, d, cb], ym_s.at[d, h, cb], ym_r.at[d, h, cb])
                    red[h, cb, yy(o), half] += ymid[h, d, cb]
                    y_acc(h, cb, d).start()

    def y_finish(t):
        for e in range(ents):
            h, cb = place(t, e)

            @pl.when(exists(t, 0, e))
            def _():
                for d in range(2):
                    half, other = (U, T)[d], (T, U)[d]
                    arrived(ydst.at[h, d, cb, half], yo_s.at[d, h, cb], yo_r.at[d, h, cb])
                    arrived(ydst.at[h, d, cb, other], ya_s.at[d, h, cb], ya_r.at[d, h, cb])
                val = red[h, cb, y] + ydst[h, 0, cb] + ydst[h, 1, cb]
                shape = (HALF, BLOCK)
                i = (rows * lax.div(h, 2) + y) * BLOCK + lax.rem(h, 2) * HALF + lax.broadcasted_iota(jnp.int32, shape, 0)
                j = (cols * cb + pos) * BLOCK + lax.broadcasted_iota(jnp.int32, shape, 1)
                c_ref[pl.ds(pl.multiple_of(h * HALF, HALF), HALF), pl.ds(pl.multiple_of(cb * BLOCK, BLOCK), BLOCK)] = (
                    jnp.where(i >= j, val, 0.0).astype(c_ref.dtype))

    def y_sent(t):
        for e in range(ents):
            h, cb = place(t, e)
            for d in range(2):
                o, half, other = (1, rows - 1)[d], (U, T)[d], (T, U)[d]

                @pl.when(exists(t, 2, e))
                def _():
                    left_us(red.at[h, cb, yy(2), other], ym_s.at[d, h, cb], ym_r.at[d, h, cb])

                @pl.when(exists(t, o, e))
                def _():
                    left_us(red.at[h, cb, yy(o), half], yo_s.at[d, h, cb], yo_r.at[d, h, cb])
                    left_us(red.at[h, cb, yy(o), other], ya_s.at[d, h, cb], ya_r.at[d, h, cb])

    def loop(lo, hi, f):
        def body(i, _):
            f(i)
            return 0
        lax.fori_loop(lo, hi, body, 0)

    both(relay_out, 0)
    both(relay_out, 1)
    both(direct, 0)
    loop(0, steps, lambda h: own(h).start())
    c_ref[...] = jnp.zeros_like(c_ref)
    pass_on(0)
    both(relay_out, 2)
    both(direct, 1)
    pass_on(1)
    both(relay_out, 3)
    items = 3 * steps // 2

    def step(t):
        w, kind = lax.div(t, 3), lax.rem(t, 3)
        h = 2 * w + kind

        @pl.when(kind < 2)
        def _():
            have(h)
            to_twin(h).start()

            @pl.when(h + 2 < steps)
            def _():
                pass_on(h + 2)
                both(direct, h + 2)

            @pl.when(h + 4 < steps)
            def _():
                both(relay_out, h + 4)

        @pl.when(t >= 2)
        def _():
            x_finish(t - 2)
            give_credit()

        @pl.when(t >= 1)
        def _():
            x_pass_on(t - 1)

        @pl.when(t >= 2)
        def _():
            x_sent(t - 2)

        @pl.when(kind < 2)
        def _():
            arrived(twin_rows(h, width), core_s.at[h], core_r.at[h])
        compute(t, 2)

        @pl.when(t >= 2)
        def _():
            take_credit()
        x_send_mid(t)
        compute(t, 1)
        x_send_own(t, 0)
        compute(t, chips - 1)
        x_send_own(t, 1)
        compute(t, 0)

    loop(0, items, step)

    early = items - 2
    loop(0, early, y_send)
    x_finish(items - 2)
    x_pass_on(items - 1)
    y_send(items - 2)
    loop(0, early, y_pass_on)
    y_pass_on(items - 2)
    x_finish(items - 1)
    y_send(items - 1)
    loop(0, early, y_finish)
    y_finish(items - 2)
    y_pass_on(items - 1)
    y_finish(items - 1)

    def drain(h):
        for d in range(2):
            left_us(a_piece(h, yy(1), 0, width), d_s.at[d, h], d_r.at[d, h])
            left_us(a_piece(h, yy(2), 0, half_w), r_s.at[d, h], r_r.at[d, h])
            left_us(relay.at[d, h], f_s.at[d, h], f_r.at[d, h])
        left_us(twin_rows(h, 0), core_s.at[h], core_r.at[h])

    x_sent(items - 2)
    x_sent(items - 1)
    loop(0, steps, drain)
    loop(0, items, y_sent)


def solution(mesh):
    rows, cols = mesh.shape["row"], mesh.shape["col"]

    def local_fn(a_local):
        local_rows, m_local = a_local.shape
        steps, waves = local_rows // HALF, local_rows // BLOCK
        width = m_local // rows
        chips = cols // 2
        cbs = local_rows * rows // (BLOCK * cols)
        dma = pltpu.SemaphoreType.DMA
        c, _ = pl.pallas_call(
            functools.partial(kernel, rows, cols),
            out_shape=(
                jax.ShapeDtypeStruct((local_rows, cbs * BLOCK), a_local.dtype),
                jax.ShapeDtypeStruct((2, steps, HALF, width // 2), a_local.dtype),
            ),
            in_specs=[pl.BlockSpec(memory_space=pltpu.HBM)],
            out_specs=(pl.BlockSpec(memory_space=pltpu.VMEM), pl.BlockSpec(memory_space=pltpu.HBM)),
            scratch_shapes=[
                pltpu.VMEM((waves, rows, BLOCK, 2 * width), a_local.dtype),
                pltpu.VMEM((2, chips - 1, cbs, rows, HALF, BLOCK), F32),
                pltpu.VMEM((2, 2, cbs, 2, HALF, BLOCK), F32),
                pltpu.VMEM((2, 2, cbs, rows, HALF, BLOCK), F32),
                pltpu.VMEM((steps, cbs, rows, HALF, BLOCK), F32),
                pltpu.VMEM((steps, 2, cbs, QUART, BLOCK), F32),
                pltpu.VMEM((steps, 2, cbs, HALF, BLOCK), F32),
            ] + [dma((2, steps))] * 6 + [dma((steps,))] * 3 + [dma((2, 2, cbs))] * 6
            + [dma((2, steps, cbs))] * 6 + [pltpu.SemaphoreType.REGULAR((2,))],
            compiler_params=pltpu.CompilerParams(
                collective_id=0, has_side_effects=True, vmem_limit_bytes=67043328),
        )(a_local)
        return c

    spec = P(("batch", "row"), "col")
    return jax.shard_map(local_fn, mesh=mesh, in_specs=(spec,), out_specs=spec, check_vma=False)
```

```python
import functools

import jax
import jax.numpy as jnp
from jax import lax
from jax.experimental import pallas as pl
from jax.experimental.pallas import tpu as pltpu
from jax.sharding import PartitionSpec as P

BLOCK = 256
HALF = BLOCK // 2
QUART = BLOCK // 4
MESH = pl.DeviceIdType.MESH
F32 = jnp.float32
START = 8
TAIL = (
    "S5", "H9", "p7", "C8", "S2", "G9", "f6", "C9", "S3", "H10", "f7", "S7", "S4", "P3", "p8", "S6", "p9",
    "C10", "P5", "f8", "Z0", "F5", "P4", "P2", "p10", "f9", "F3", "S8", "Z1", "P6", "F2", "P8", "S9", "f10",
    "S10", "Z2", "P9", "Z3", "F4", "P10", "P7", "F9", "F8", "F6", "F10", "Z4", "F7",
)


def kernel(rows, cols, a_ref, c_ref, relay, xin, part, xmid, xdst, red, ymid, ydst, fin,
           d_s, d_r, r_s, r_r, f_s, f_r, loc_s, core_s, core_r,
           xm_s, xm_r, xo_s, xo_r, xa_s, xa_r, ym_s, ym_r, yo_s, yo_r, ya_s, ya_r,
           zm_s, zm_r, zo_s, zo_r, za_s, za_r, wm_s, wm_r, wo_s, wo_r, wa_s, wa_r, fin_s, fin_r, credit):
    chips = cols // 2
    y = lax.axis_index("row")
    pos = lax.axis_index("col")
    x, core = lax.div(pos, 2), lax.rem(pos, 2)
    local_rows, m_local = a_ref.shape
    width = m_local // rows
    half_w = width // 2
    steps = local_rows // HALF
    items = 3 * steps // 2
    last = steps // 2 - 1
    late = steps - steps // 2
    slots, ents = part.shape[0], part.shape[2]

    def div(p, q):
        return p // q if isinstance(p, int) else lax.div(p, q)

    def rem(p, q):
        return p % q if isinstance(p, int) else lax.rem(p, q)

    def when(test, f):
        if isinstance(test, bool):
            if test:
                f()
        else:
            pl.when(test)(f)

    def yy(o):
        return lax.rem(y + o, rows)

    def xx(o):
        return lax.rem(x + o, chips)

    up, down = {"row": yy(1)}, {"row": yy(rows - 1)}
    right, left = {"col": 2 * xx(1) + core}, {"col": 2 * xx(chips - 1) + core}
    across = {"col": 2 * xx(2) + core}
    twin = {"col": 2 * x + 1 - core}
    ydev, xdev = (up, down), (right, left)

    def remote(src, dst, s, r, dev):
        return pltpu.make_async_remote_copy(
            src_ref=src, dst_ref=dst, send_sem=s, recv_sem=r, device_id=dev, device_id_type=MESH)

    def arrived(dst, s, r):
        remote(dst, dst, s, r, twin).wait_recv()

    def left_us(src, s, r):
        remote(src, src, s, r, twin).wait_send()

    def signal(sem, dev):
        pl.semaphore_signal(sem, inc=1, device_id=dev, device_id_type=MESH)

    barrier = pltpu.get_barrier_semaphore()
    for dev in (up, down, right, left, across, twin):
        signal(barrier, dev)
    pl.semaphore_wait(barrier, 6)

    def half_rows(h):
        return pl.ds(pl.multiple_of(rem(h, 2) * HALF, HALF), HALF)

    def a_piece(h, owner, off, size):
        return a_ref.at[pl.ds(pl.multiple_of(h * HALF, HALF), HALF),
                        pl.ds(pl.multiple_of(owner * width + off, 128), size)]

    def x_piece(h, group, off, size):
        return xin.at[div(h, 2), group, half_rows(h), pl.ds(off, size)]

    def direct(h, d):
        return remote(a_piece(h, yy(1 if d == 0 else rows - 1), 0, width), x_piece(h, y, 0, width),
                      d_s.at[d, h], d_r.at[d, h], ydev[d])

    def relay_out(h, d):
        return remote(a_piece(h, yy(2), d * half_w, half_w), relay.at[d, h], r_s.at[d, h], r_r.at[d, h], ydev[d])

    def forward(h, d):
        return remote(relay.at[d, h], x_piece(h, yy(rows - 1 if d == 0 else 1), d * half_w, half_w),
                      f_s.at[d, h], f_r.at[d, h], ydev[d])

    def own(h):
        return pltpu.make_async_copy(a_piece(h, y, 0, width), x_piece(h, y, 0, width), loc_s.at[h])

    def twin_rows(h, off):
        return xin.at[div(h, 2), :, half_rows(h), pl.ds(off, width)]

    def to_twin(h):
        return remote(twin_rows(h, 0), twin_rows(h, width), core_s.at[h], core_r.at[h], twin)

    def both(f, h):
        for d in range(2):
            f(h, d).start()

    def pass_on(h):
        for d in range(2):
            arrived(relay.at[d, h], r_s.at[d, h], r_r.at[d, h])
        both(forward, h)

    def split(t):
        w, kind = div(t, 3), rem(t, 3)
        return w, kind, div(kind, 2)

    def choose(own_cols, before, inside):
        if isinstance(own_cols, int):
            return inside if own_cols else before
        return ((own_cols == 0) & before) | ((own_cols == 1) & inside)

    def place(t, e):
        w, kind, own_cols = split(t)
        return 2 * w + (1 - own_cols) * kind + own_cols * e, (1 - own_cols) * e + own_cols * div(2 * w, chips)

    def spot(t, e):
        h, cb = place(t, e)
        return h + late * cb

    def moved(t):
        return isinstance(t, int) and t // 3 == last and t % 3 < 2

    def column(t, o, e):
        return chips * place(t, e)[1] + xx(o + 2 * e if moved(t) else o)

    def low(t, o, e):
        w, _, own_cols = split(t)
        m = column(t, o, e)
        return choose(own_cols, m < 2 * w, m == 2 * w)

    def high(t, o, e):
        w, _, own_cols = split(t)
        m = column(t, o, e)
        return choose(own_cols, m < 2 * w, lax.div(m, 2) == w)

    A, B = pl.ds(0, 2), pl.ds(2, 2)

    def product(w, h, m):
        j = 2 * m + core
        lhs = xin[w, :, half_rows(h), :].reshape(rows * HALF, 2 * width)
        rhs = xin[lax.div(j, rows), lax.rem(j, rows)]
        val = lax.dot_general(lhs, rhs, (((1,), (1,)), ((), ())), preferred_element_type=F32)
        return val.reshape(rows, HALF, BLOCK)

    def x_mid(t, e, d):
        sl = rem(t, slots)
        return remote(part.at[sl, 1, e, (A, B)[d]], xmid.at[sl, d, e],
                      xm_s.at[d, sl, e], xm_r.at[d, sl, e], xdev[d])

    def x_own(t, e, d):
        sl, half = rem(t, slots), (B, A)[d]
        return remote(part.at[sl, 2 * d, e, half], xdst.at[sl, d, e, half],
                      xo_s.at[d, sl, e], xo_r.at[d, sl, e], xdev[d])

    def x_acc(t, e, d):
        sl, half = rem(t, slots), (A, B)[d]
        return remote(part.at[sl, 2 * d, e, half], xdst.at[sl, d, e, half],
                      xa_s.at[d, sl, e], xa_r.at[d, sl, e], xdev[d])

    def x_send_mid(t):
        for e in range(ents):
            when(low(t, 2, e), lambda: x_mid(t, e, 0).start())
            when(high(t, 2, e), lambda: x_mid(t, e, 1).start())

    def x_send_own(t, d):
        for e in range(ents):
            when(high(t, 1, e) if d == 0 else low(t, chips - 1, e), lambda: x_own(t, e, d).start())

    def x_pass_on(t):
        sl = rem(t, slots)
        for e in range(ents):
            for d, o, half, test in ((0, 1, A, low), (1, chips - 1, B, high)):
                def one():
                    arrived(xmid.at[sl, d, e], xm_s.at[d, sl, e], xm_r.at[d, sl, e])
                    part[sl, 2 * d, e, half] += xmid[sl, d, e]
                    x_acc(t, e, d).start()
                when(test(t, o, e), one)

    def x_finish(t):
        sl = rem(t, slots)
        for e in range(ents):
            ix = spot(t, e)

            def first():
                arrived(xdst.at[sl, 0, e, A], xa_s.at[0, sl, e], xa_r.at[0, sl, e])
                arrived(xdst.at[sl, 1, e, A], xo_s.at[1, sl, e], xo_r.at[1, sl, e])
                red[ix, A] = red[ix, A] + xdst[sl, 0, e, A] + xdst[sl, 1, e, A]

            def second():
                arrived(xdst.at[sl, 0, e, B], xo_s.at[0, sl, e], xo_r.at[0, sl, e])
                arrived(xdst.at[sl, 1, e, B], xa_s.at[1, sl, e], xa_r.at[1, sl, e])
                red[ix, B] = red[ix, B] + xdst[sl, 0, e, B] + xdst[sl, 1, e, B]
            when(low(t, 0, e), first)
            when(high(t, 0, e), second)
        if not isinstance(t, int) or t + slots < items:
            signal(credit.at[0], left)
            signal(credit.at[1], right)
        if isinstance(t, int) and t + slots == items - 1:
            signal(credit.at[2], up)
            signal(credit.at[3], down)

    def x_sent(t):
        sl = rem(t, slots)
        for e in range(ents):
            for o, d, half, s, r, test in (
                    (2, 0, A, xm_s, xm_r, low), (2, 1, B, xm_s, xm_r, high),
                    (1, 0, B, xo_s, xo_r, high), (chips - 1, 1, A, xo_s, xo_r, low),
                    (1, 0, A, xa_s, xa_r, low), (chips - 1, 1, B, xa_s, xa_r, high)):
                when(test(t, o, e), lambda: left_us(part.at[sl, o - 1, e, half], s.at[d, sl, e], r.at[d, sl, e]))

    def take_credit(first):
        pl.semaphore_wait(credit.at[first], 1)
        pl.semaphore_wait(credit.at[first + 1], 1)

    def compute(t):
        w, kind, _ = split(t)
        sl = rem(t, slots)

        def twin_in():
            h = 2 * w + kind
            arrived(twin_rows(h, width), core_s.at[h], core_r.at[h])
        when(kind < 2, twin_in)
        when(t >= slots, lambda: x_sent(t - slots))

        def one(i, _):
            n, e = lax.div(i, 2), lax.rem(i, 2)
            o = lax.rem(2 + 3 * n + 3 * lax.div(n, 2) + 2 * lax.div(n, 3), chips)
            m = column(t, o, e)

            @pl.when(high(t, o, e))
            def _():
                h, cb = place(t, e)
                val = product(w, h, m)

                @pl.when(o == 0)
                def _():
                    red[h + late * cb] = val

                @pl.when(o > 0)
                def _():
                    part[sl, o - 1, e] = val

            @pl.when(i == 1)
            def _():
                when(t >= slots, lambda: take_credit(0))
                x_send_mid(t)

            @pl.when(i == 3)
            def _():
                x_send_own(t, 0)

            @pl.when(i == 5)
            def _():
                x_send_own(t, 1)
            return 0

        lax.fori_loop(0, 2 * chips, one, 0)

    T, U = pl.ds(0, QUART), pl.ds(QUART, QUART)
    ahead = (1, rows - 1)

    def exists(t, o, e):
        w, _, own_cols = split(t)
        m = column(t, 0, e)
        return choose(own_cols, m < 2 * w, (lax.div(m, 2) == w) & (rows * w + yy(o) >= 2 * m + core))

    def y_mid(ix, d):
        return remote(red.at[ix, yy(2), (T, U)[d]], ymid.at[ix, d], ym_s.at[d, ix], ym_r.at[d, ix], ydev[d])

    def y_own(ix, d):
        half = (U, T)[d]
        return remote(red.at[ix, yy(ahead[d]), half], ydst.at[ix, d, half], yo_s.at[d, ix], yo_r.at[d, ix], ydev[d])

    def y_acc(ix, d):
        half = (T, U)[d]
        return remote(red.at[ix, yy(ahead[d]), half], ydst.at[ix, d, half], ya_s.at[d, ix], ya_r.at[d, ix], ydev[d])

    def y_send(t):
        for e in range(ents):
            when(exists(t, 2, e), lambda: [y_mid(spot(t, e), d).start() for d in range(2)] and None)
        for e in range(ents):
            for d in range(2):
                when(exists(t, ahead[d], e), lambda: y_own(spot(t, e), d).start())

    def y_pass_on(t):
        for e in range(ents):
            ix = spot(t, e)
            for d in range(2):
                o, half = ahead[d], (T, U)[d]

                def one():
                    arrived(ymid.at[ix, d], ym_s.at[d, ix], ym_r.at[d, ix])
                    red[ix, yy(o), half] += ymid[ix, d]
                    y_acc(ix, d).start()
                when(exists(t, o, e), one)

    def rounded(h, m, val):
        i = (rows * div(h, 2) + y) * BLOCK + rem(h, 2) * HALF + lax.broadcasted_iota(jnp.int32, val.shape, 0)
        j = (2 * m + core) * BLOCK + lax.broadcasted_iota(jnp.int32, val.shape, 1)
        return jnp.where(i >= j, val, 0.0).astype(c_ref.dtype)

    def result(h, cb):
        return (pl.ds(pl.multiple_of(h * HALF, HALF), HALF), pl.ds(pl.multiple_of(cb * BLOCK, BLOCK), BLOCK))

    def to_owner(s):
        return remote(fin.at[0, s], fin.at[1, s], fin_s.at[s], fin_r.at[s], across)

    def y_finish(t):
        for e in range(ents):
            h, cb = place(t, e)
            ix = spot(t, e)

            def one():
                for d in range(2):
                    half, other = (U, T)[d], (T, U)[d]
                    arrived(ydst.at[ix, d, half], yo_s.at[d, ix], yo_r.at[d, ix])
                    arrived(ydst.at[ix, d, other], ya_s.at[d, ix], ya_r.at[d, ix])
                val = rounded(h, column(t, 0, e), red[ix, y] + ydst[ix, 0] + ydst[ix, 1])
                if moved(t) and e == 1:
                    fin[0, t % 3] = val
                    to_owner(t % 3).start()
                else:
                    c_ref[result(h, cb)] = val
            when(exists(t, 0, e), one)

    def from_opposite():
        for s in range(2):
            def one():
                arrived(fin.at[1, s], fin_s.at[s], fin_r.at[s])
                c_ref[result(2 * last + s, 1)] = fin[1, s]
            when(chips + x < 2 * last, one)

    def y_sent(t):
        for e in range(ents):
            ix = spot(t, e)
            for d in range(2):
                o, half, other = ahead[d], (U, T)[d], (T, U)[d]

                def sides():
                    left_us(red.at[ix, yy(o), half], yo_s.at[d, ix], yo_r.at[d, ix])
                    left_us(red.at[ix, yy(o), other], ya_s.at[d, ix], ya_r.at[d, ix])
                when(exists(t, 2, e), lambda: left_us(red.at[ix, yy(2), other], ym_s.at[d, ix], ym_r.at[d, ix]))
                when(exists(t, o, e), sides)

    zs = (items - 1) % slots
    pairs = [(g, e) for g in range(2) for e in range(2)]

    def z_exists(g, o):
        return yy(o) >= 2 * g + core

    def z_mid(g, e, d):
        return remote(part.at[zs, g, e, yy(2), (T, U)[d]], xmid.at[zs, d, e, g, T],
                      zm_s.at[d, g, e], zm_r.at[d, g, e], ydev[d])

    def z_side(g, e, d, half, s, r):
        return remote(part.at[zs, g, e, yy(ahead[d]), half], xdst.at[zs, d, e, g, half],
                      s.at[d, g, e], r.at[d, g, e], ydev[d])

    def z_own(g, e, d):
        return z_side(g, e, d, (U, T)[d], zo_s, zo_r)

    def z_acc(g, e, d):
        return z_side(g, e, d, (T, U)[d], za_s, za_r)

    def away(g):
        return lax.rem((2 * last + g) % chips + chips - x, chips)

    def w_mid(g, e, d):
        return remote(part.at[zs, g, e, y, (T, U)[d]], xmid.at[zs, d, e, 0, U], wm_s.at[d, e], wm_r.at[d, e], xdev[d])

    def w_side(g, e, d, half, s, r):
        return remote(part.at[zs, g, e, y, half], xdst.at[zs, d, e, 2, half], s.at[d, e], r.at[d, e], xdev[d])

    def w_own(g, e, d):
        return w_side(g, e, d, (U, T)[d], wo_s, wo_r)

    def w_acc(g, e, d):
        return w_side(g, e, d, (T, U)[d], wa_s, wa_r)

    def z_compute():
        x_sent(items - 1 - slots)

        def one(i, _):
            g, e = lax.div(i, 2), lax.rem(i, 2)
            part[zs, g, e] = product(last, e, 2 * last + g)
            return 0
        lax.fori_loop(0, 4, one, 0)
        take_credit(2)
        for g, e in pairs:
            when(z_exists(g, 2), lambda: [z_mid(g, e, d).start() for d in range(2)] and None)
        for g, e in pairs:
            for d in range(2):
                when(z_exists(g, ahead[d]), lambda: z_own(g, e, d).start())

    def z_pass_on():
        for g, e in pairs:
            for d in range(2):
                half = (T, U)[d]

                def one():
                    arrived(xmid.at[zs, d, e, g, T], zm_s.at[d, g, e], zm_r.at[d, g, e])
                    part[zs, g, e, yy(ahead[d]), half] += xmid[zs, d, e, g, T]
                    z_acc(g, e, d).start()
                when(z_exists(g, ahead[d]), one)

    def z_turn():
        take_credit(0)
        for g, e in pairs:
            def one():
                for d in range(2):
                    half, other = (U, T)[d], (T, U)[d]
                    arrived(xdst.at[zs, d, e, g, half], zo_s.at[d, g, e], zo_r.at[d, g, e])
                    arrived(xdst.at[zs, d, e, g, other], za_s.at[d, g, e], za_r.at[d, g, e])
                part[zs, g, e, y] = part[zs, g, e, y] + xdst[zs, 0, e, g] + xdst[zs, 1, e, g]
                pl.when(away(g) == 2)(lambda: [w_mid(g, e, d).start() for d in range(2)] and None)
                pl.when(away(g) == 1)(lambda: w_own(g, e, 0).start())
                pl.when(away(g) == chips - 1)(lambda: w_own(g, e, 1).start())
            when(z_exists(g, 0), one)

    def w_pass_on():
        for g, e in pairs:
            for d in range(2):
                half = (T, U)[d]

                def one():
                    arrived(xmid.at[zs, d, e, 0, U], wm_s.at[d, e], wm_r.at[d, e])
                    part[zs, g, e, y, half] += xmid[zs, d, e, 0, U]
                    w_acc(g, e, d).start()
                when(z_exists(g, 0) & (away(g) == (1, chips - 1)[d]), one)

    def w_finish():
        for g, e in pairs:
            def one():
                for d in range(2):
                    half, other = (U, T)[d], (T, U)[d]
                    arrived(xdst.at[zs, d, e, 2, half], wo_s.at[d, e], wo_r.at[d, e])
                    arrived(xdst.at[zs, d, e, 2, other], wa_s.at[d, e], wa_r.at[d, e])
                val = part[zs, g, e, y] + xdst[zs, 0, e, 2] + xdst[zs, 1, e, 2]
                m = 2 * last + g
                c_ref[result(2 * last + e, m // chips)] = rounded(2 * last + e, m, val)
            when(z_exists(g, 0) & (away(g) == 0), one)

    def z_sent():
        for g, e in pairs:
            for d in range(2):
                half, other = (U, T)[d], (T, U)[d]

                def sides():
                    left_us(part.at[zs, g, e, yy(ahead[d]), half], zo_s.at[d, g, e], zo_r.at[d, g, e])
                    left_us(part.at[zs, g, e, yy(ahead[d]), other], za_s.at[d, g, e], za_r.at[d, g, e])

                def w_sides():
                    left_us(part.at[zs, g, e, y, half], wo_s.at[d, e], wo_r.at[d, e])
                    left_us(part.at[zs, g, e, y, other], wa_s.at[d, e], wa_r.at[d, e])
                when(z_exists(g, 2), lambda: left_us(part.at[zs, g, e, yy(2), other], zm_s.at[d, g, e], zm_r.at[d, g, e]))
                when(z_exists(g, ahead[d]), sides)
                when(z_exists(g, 0) & (away(g) == 2),
                     lambda: left_us(part.at[zs, g, e, y, other], wm_s.at[d, e], wm_r.at[d, e]))
                when(z_exists(g, 0) & (away(g) == (1, chips - 1)[d]), w_sides)

    def half_of(t):
        return 2 * div(t, 3) + rem(t, 3)

    def have(t):
        h = half_of(t)
        own(h).wait()
        for d in range(2):
            arrived(x_piece(h, yy(rows - 1 if d == 0 else 1), 0, width), d_s.at[d, h], d_r.at[d, h])
            arrived(x_piece(h, yy(2), d * half_w, half_w), f_s.at[d, h], f_r.at[d, h])
        to_twin(h).start()

    def more(t):
        h = half_of(t)
        when(h + 3 < steps, lambda: both(relay_out, h + 3))

        def forth():
            pass_on(h + 2)
            both(direct, h + 2)
        when(h + 2 < steps, forth)

    def loop(lo, hi, f):
        def body(i, _):
            f(i)
            return 0
        lax.fori_loop(lo, hi, body, 0)

    both(relay_out, 0)
    both(relay_out, 1)
    pass_on(0)
    both(direct, 0)
    both(relay_out, 2)
    loop(0, steps, lambda h: own(h).start())
    c_ref[...] = jnp.zeros_like(c_ref)
    pass_on(1)
    both(direct, 1)

    def step(t):
        when(rem(t, 3) < 2, lambda: have(t))
        compute(t)
        when(rem(t, 3) < 2, lambda: more(t))
        when(t >= 1, lambda: x_pass_on(t - 1))
        when(t >= 2, lambda: x_finish(t - 2))

    loop(0, START, step)

    acts = {"H": have, "G": more, "C": compute, "p": x_pass_on, "f": x_finish, "S": y_send, "P": y_pass_on,
            "F": y_finish, "Z": lambda n: (z_compute, z_pass_on, z_turn, w_pass_on, w_finish)[n]()}
    for act in TAIL:
        acts[act[0]](int(act[1:]))
    from_opposite()

    def drain(h):
        for d in range(2):
            left_us(a_piece(h, yy(1), 0, width), d_s.at[d, h], d_r.at[d, h])
            left_us(a_piece(h, yy(2), 0, half_w), r_s.at[d, h], r_r.at[d, h])
            left_us(relay.at[d, h], f_s.at[d, h], f_r.at[d, h])
        left_us(twin_rows(h, 0), core_s.at[h], core_r.at[h])

    loop(0, steps, drain)
    z_sent()
    for t in range(items - slots, items - 1):
        x_sent(t)
    for s in range(2):
        when(chips + xx(2) < 2 * last, lambda: left_us(fin.at[0, s], fin_s.at[s], fin_r.at[s]))
    loop(0, items - 3, y_sent)
    for t in range(items - 3, items - 1):
        y_sent(t)


def solution(mesh):
    rows, cols = mesh.shape["row"], mesh.shape["col"]

    def local_fn(a_local):
        local_rows, m_local = a_local.shape
        steps, waves = local_rows // HALF, local_rows // BLOCK
        width = m_local // rows
        chips = cols // 2
        cbs = local_rows * rows // (BLOCK * cols)
        slots, spots = 3, steps + steps // 2
        dma = pltpu.SemaphoreType.DMA
        c, _ = pl.pallas_call(
            functools.partial(kernel, rows, cols),
            out_shape=(
                jax.ShapeDtypeStruct((local_rows, cbs * BLOCK), a_local.dtype),
                jax.ShapeDtypeStruct((2, steps, HALF, width // 2), a_local.dtype),
            ),
            in_specs=[pl.BlockSpec(memory_space=pltpu.HBM)],
            out_specs=(pl.BlockSpec(memory_space=pltpu.VMEM), pl.BlockSpec(memory_space=pltpu.HBM)),
            scratch_shapes=[
                pltpu.VMEM((waves, rows, BLOCK, 2 * width), a_local.dtype),
                pltpu.VMEM((slots, chips - 1, cbs, rows, HALF, BLOCK), F32),
                pltpu.VMEM((slots, 2, cbs, 2, HALF, BLOCK), F32),
                pltpu.VMEM((slots, 2, cbs, rows, HALF, BLOCK), F32),
                pltpu.VMEM((spots, rows, HALF, BLOCK), F32),
                pltpu.VMEM((spots, 2, QUART, BLOCK), F32),
                pltpu.VMEM((spots, 2, HALF, BLOCK), F32),
                pltpu.VMEM((2, 2, HALF, BLOCK), a_local.dtype),
            ] + [dma((2, steps))] * 6 + [dma((steps,))] * 3 + [dma((2, slots, cbs))] * 6 + [dma((2, spots))] * 6
            + [dma((2, 2, 2))] * 6 + [dma((2, 2))] * 6 + [dma((2,))] * 2 + [pltpu.SemaphoreType.REGULAR((4,))],
            compiler_params=pltpu.CompilerParams(
                collective_id=0, has_side_effects=True, vmem_limit_bytes=67043328),
        )(a_local)
        return c

    spec = P(("batch", "row"), "col")
    return jax.shard_map(local_fn, mesh=mesh, in_specs=(spec,), out_specs=spec, check_vma=False)
```

```python
import functools

import jax
import jax.numpy as jnp
from jax import lax
from jax.experimental import pallas as pl
from jax.experimental.pallas import tpu as pltpu
from jax.sharding import PartitionSpec as P

BLOCK = 256
HALF = BLOCK // 2
QUART = BLOCK // 4
MESH = pl.DeviceIdType.MESH
F32 = jnp.float32
START = 6
TAIL = (
    "p5", "H6", "G6", "C6", "H7", "f4", "f5", "p6", "C7", "G7", "f6", "C8", "H9", "S4", "p7", "C9", "f7",
    "S3", "G9", "p9b", "S6", "H10", "P3", "P6", "p8", "S2", "p9a", "S7", "P2", "C10", "P7", "P4", "f8", "S8",
    "Z0", "f9a", "p10b", "S5", "P8", "Z1", "f9b", "S9a", "F6", "P5", "S9b", "F2", "p10a", "P9a", "f10b",
    "F5", "S10b", "P10b", "Z2", "P9b", "f10a", "S10a", "F8", "F10b", "F9b", "Z3", "F7", "F9a", "P10a", "F3",
    "F10a", "Z4", "F4",
)


def kernel(rows, cols, a_ref, c_ref, relay, xin, part, xmid, xdst, red, ymid, ydst, fin,
           d_s, d_r, r_s, r_r, f_s, f_r, loc_s, core_s, core_r,
           xm_s, xm_r, xo_s, xo_r, xa_s, xa_r, ym_s, ym_r, yo_s, yo_r, ya_s, ya_r,
           zm_s, zm_r, zo_s, zo_r, za_s, za_r, wm_s, wm_r, wo_s, wo_r, wa_s, wa_r, fin_s, fin_r, credit):
    chips = cols // 2
    y = lax.axis_index("row")
    pos = lax.axis_index("col")
    x, core = lax.div(pos, 2), lax.rem(pos, 2)
    local_rows, m_local = a_ref.shape
    width = m_local // rows
    half_w = width // 2
    steps = local_rows // HALF
    items = 3 * steps // 2
    last = steps // 2 - 1
    late = steps - steps // 2
    slots, ents = part.shape[0], part.shape[2]
    every = tuple(range(ents))

    def div(p, q):
        return p // q if isinstance(p, int) else lax.div(p, q)

    def rem(p, q):
        return p % q if isinstance(p, int) else lax.rem(p, q)

    def when(test, f):
        if isinstance(test, bool):
            if test:
                f()
        else:
            pl.when(test)(f)

    def yy(o):
        return lax.rem(y + o, rows)

    def xx(o):
        return lax.rem(x + o, chips)

    up, down = {"row": yy(1)}, {"row": yy(rows - 1)}
    right, left = {"col": 2 * xx(1) + core}, {"col": 2 * xx(chips - 1) + core}
    across = {"col": 2 * xx(2) + core}
    twin = {"col": 2 * x + 1 - core}
    ydev, xdev = (up, down), (right, left)

    def remote(src, dst, s, r, dev):
        return pltpu.make_async_remote_copy(
            src_ref=src, dst_ref=dst, send_sem=s, recv_sem=r, device_id=dev, device_id_type=MESH)

    def arrived(dst, s, r):
        remote(dst, dst, s, r, twin).wait_recv()

    def left_us(src, s, r):
        remote(src, src, s, r, twin).wait_send()

    def signal(sem, dev):
        pl.semaphore_signal(sem, inc=1, device_id=dev, device_id_type=MESH)

    barrier = pltpu.get_barrier_semaphore()
    for dev in (up, down, right, left, across, twin):
        signal(barrier, dev)
    pl.semaphore_wait(barrier, 6)

    def half_rows(h):
        return pl.ds(pl.multiple_of(rem(h, 2) * HALF, HALF), HALF)

    def a_piece(h, owner, off, size):
        return a_ref.at[pl.ds(pl.multiple_of(h * HALF, HALF), HALF),
                        pl.ds(pl.multiple_of(owner * width + off, 128), size)]

    def x_piece(h, group, off, size):
        return xin.at[div(h, 2), group, half_rows(h), pl.ds(off, size)]

    def direct(h, d):
        return remote(a_piece(h, yy(1 if d == 0 else rows - 1), 0, width), x_piece(h, y, 0, width),
                      d_s.at[d, h], d_r.at[d, h], ydev[d])

    def relay_out(h, d):
        return remote(a_piece(h, yy(2), d * half_w, half_w), relay.at[d, h], r_s.at[d, h], r_r.at[d, h], ydev[d])

    def forward(h, d):
        return remote(relay.at[d, h], x_piece(h, yy(rows - 1 if d == 0 else 1), d * half_w, half_w),
                      f_s.at[d, h], f_r.at[d, h], ydev[d])

    def own(h):
        return pltpu.make_async_copy(a_piece(h, y, 0, width), x_piece(h, y, 0, width), loc_s.at[h])

    def twin_rows(h, off):
        return xin.at[div(h, 2), :, half_rows(h), pl.ds(off, width)]

    def to_twin(h):
        return remote(twin_rows(h, 0), twin_rows(h, width), core_s.at[h], core_r.at[h], twin)

    def both(f, h):
        for d in range(2):
            f(h, d).start()

    def pass_on(h):
        for d in range(2):
            arrived(relay.at[d, h], r_s.at[d, h], r_r.at[d, h])
        both(forward, h)

    def split(t):
        w, kind = div(t, 3), rem(t, 3)
        return w, kind, div(kind, 2)

    def choose(own_cols, before, inside):
        if isinstance(own_cols, int):
            return inside if own_cols else before
        return ((own_cols == 0) & before) | ((own_cols == 1) & inside)

    def place(t, e):
        w, kind, own_cols = split(t)
        return 2 * w + (1 - own_cols) * kind + own_cols * e, (1 - own_cols) * e + own_cols * div(2 * w, chips)

    def spot(t, e):
        h, cb = place(t, e)
        return h + late * cb

    def moved(t):
        return isinstance(t, int) and t // 3 == last and t % 3 < 2

    def column(t, o, e):
        return chips * place(t, e)[1] + xx(o + 2 * e if moved(t) else o)

    def low(t, o, e):
        w, _, own_cols = split(t)
        m = column(t, o, e)
        return choose(own_cols, m < 2 * w, m == 2 * w)

    def high(t, o, e):
        w, _, own_cols = split(t)
        m = column(t, o, e)
        return choose(own_cols, m < 2 * w, lax.div(m, 2) == w)

    A, B = pl.ds(0, 2), pl.ds(2, 2)

    def product(w, h, m):
        j = 2 * m + core
        lhs = xin[w, :, half_rows(h), :].reshape(rows * HALF, 2 * width)
        rhs = xin[lax.div(j, rows), lax.rem(j, rows)]
        val = lax.dot_general(lhs, rhs, (((1,), (1,)), ((), ())), preferred_element_type=F32)
        return val.reshape(rows, HALF, BLOCK)

    def x_mid(t, e, d):
        sl = rem(t, slots)
        return remote(part.at[sl, 1, e, (A, B)[d]], xmid.at[sl, d, e],
                      xm_s.at[d, sl, e], xm_r.at[d, sl, e], xdev[d])

    def x_own(t, e, d):
        sl, half = rem(t, slots), (B, A)[d]
        return remote(part.at[sl, 2 * d, e, half], xdst.at[sl, d, e, half],
                      xo_s.at[d, sl, e], xo_r.at[d, sl, e], xdev[d])

    def x_acc(t, e, d):
        sl, half = rem(t, slots), (A, B)[d]
        return remote(part.at[sl, 2 * d, e, half], xdst.at[sl, d, e, half],
                      xa_s.at[d, sl, e], xa_r.at[d, sl, e], xdev[d])

    def x_send_mid(t):
        for e in reversed(every) if moved(t) else every:
            when(low(t, 2, e), lambda: x_mid(t, e, 0).start())
            when(high(t, 2, e), lambda: x_mid(t, e, 1).start())

    def x_send_own(t, d):
        for e in reversed(every) if moved(t) else every:
            when(high(t, 1, e) if d == 0 else low(t, chips - 1, e), lambda: x_own(t, e, d).start())

    def x_pass_on(t, es=every):
        sl = rem(t, slots)
        for e in es:
            for d, o, half, test in ((0, 1, A, low), (1, chips - 1, B, high)):
                def one():
                    arrived(xmid.at[sl, d, e], xm_s.at[d, sl, e], xm_r.at[d, sl, e])
                    part[sl, 2 * d, e, half] += xmid[sl, d, e]
                    x_acc(t, e, d).start()
                when(test(t, o, e), one)

    def x_finish(t, es=every):
        sl = rem(t, slots)
        for e in es:
            ix = spot(t, e)

            def first():
                arrived(xdst.at[sl, 0, e, A], xa_s.at[0, sl, e], xa_r.at[0, sl, e])
                arrived(xdst.at[sl, 1, e, A], xo_s.at[1, sl, e], xo_r.at[1, sl, e])
                red[ix, A] = red[ix, A] + xdst[sl, 0, e, A] + xdst[sl, 1, e, A]

            def second():
                arrived(xdst.at[sl, 0, e, B], xo_s.at[0, sl, e], xo_r.at[0, sl, e])
                arrived(xdst.at[sl, 1, e, B], xa_s.at[1, sl, e], xa_r.at[1, sl, e])
                red[ix, B] = red[ix, B] + xdst[sl, 0, e, B] + xdst[sl, 1, e, B]
            when(low(t, 0, e), first)
            when(high(t, 0, e), second)
        if not isinstance(t, int) or t + slots < items:
            signal(credit.at[0], left)
            signal(credit.at[1], right)
        if isinstance(t, int) and t + slots == items - 1:
            signal(credit.at[2], up)
            signal(credit.at[3], down)

    def x_sent(t):
        sl = rem(t, slots)
        for e in range(ents):
            for o, d, half, s, r, test in (
                    (2, 0, A, xm_s, xm_r, low), (2, 1, B, xm_s, xm_r, high),
                    (1, 0, B, xo_s, xo_r, high), (chips - 1, 1, A, xo_s, xo_r, low),
                    (1, 0, A, xa_s, xa_r, low), (chips - 1, 1, B, xa_s, xa_r, high)):
                when(test(t, o, e), lambda: left_us(part.at[sl, o - 1, e, half], s.at[d, sl, e], r.at[d, sl, e]))

    def take_credit(first):
        pl.semaphore_wait(credit.at[first], 1)
        pl.semaphore_wait(credit.at[first + 1], 1)

    def compute(t):
        w, kind, _ = split(t)
        sl = rem(t, slots)

        def twin_in():
            h = 2 * w + kind
            arrived(twin_rows(h, width), core_s.at[h], core_r.at[h])
        when(kind < 2, twin_in)
        when(t >= slots, lambda: x_sent(t - slots))

        def one(i, _):
            n, e = lax.div(i, 2), 1 - lax.rem(i, 2) if moved(t) else lax.rem(i, 2)
            o = lax.rem(2 + 3 * n + 3 * lax.div(n, 2) + 2 * lax.div(n, 3), chips)
            m = column(t, o, e)

            @pl.when(high(t, o, e))
            def _():
                h, cb = place(t, e)
                val = product(w, h, m)

                @pl.when(o == 0)
                def _():
                    red[h + late * cb] = val

                @pl.when(o > 0)
                def _():
                    part[sl, o - 1, e] = val

            @pl.when(i == 1)
            def _():
                when(t >= slots, lambda: take_credit(0))
                x_send_mid(t)

            @pl.when(i == 3)
            def _():
                x_send_own(t, 0)

            @pl.when(i == 5)
            def _():
                x_send_own(t, 1)
            return 0

        lax.fori_loop(0, 2 * chips, one, 0)

    T, U = pl.ds(0, QUART), pl.ds(QUART, QUART)
    ahead = (1, rows - 1)

    def exists(t, o, e):
        w, _, own_cols = split(t)
        m = column(t, 0, e)
        return choose(own_cols, m < 2 * w, (lax.div(m, 2) == w) & (rows * w + yy(o) >= 2 * m + core))

    def y_mid(ix, d):
        return remote(red.at[ix, yy(2), (T, U)[d]], ymid.at[ix, d], ym_s.at[d, ix], ym_r.at[d, ix], ydev[d])

    def y_own(ix, d):
        half = (U, T)[d]
        return remote(red.at[ix, yy(ahead[d]), half], ydst.at[ix, d, half], yo_s.at[d, ix], yo_r.at[d, ix], ydev[d])

    def y_acc(ix, d):
        half = (T, U)[d]
        return remote(red.at[ix, yy(ahead[d]), half], ydst.at[ix, d, half], ya_s.at[d, ix], ya_r.at[d, ix], ydev[d])

    def y_send(t, es=every):
        for e in es:
            when(exists(t, 2, e), lambda: [y_mid(spot(t, e), d).start() for d in range(2)] and None)
        for e in es:
            for d in range(2):
                when(exists(t, ahead[d], e), lambda: y_own(spot(t, e), d).start())

    def y_pass_on(t, es=every):
        for e in es:
            ix = spot(t, e)
            for d in range(2):
                o, half = ahead[d], (T, U)[d]

                def one():
                    arrived(ymid.at[ix, d], ym_s.at[d, ix], ym_r.at[d, ix])
                    red[ix, yy(o), half] += ymid[ix, d]
                    y_acc(ix, d).start()
                when(exists(t, o, e), one)

    def rounded(h, m, val):
        i = (rows * div(h, 2) + y) * BLOCK + rem(h, 2) * HALF + lax.broadcasted_iota(jnp.int32, val.shape, 0)
        j = (2 * m + core) * BLOCK + lax.broadcasted_iota(jnp.int32, val.shape, 1)
        return jnp.where(i >= j, val, 0.0).astype(c_ref.dtype)

    def result(h, cb):
        return (pl.ds(pl.multiple_of(h * HALF, HALF), HALF), pl.ds(pl.multiple_of(cb * BLOCK, BLOCK), BLOCK))

    def to_owner(s):
        return remote(fin.at[0, s], fin.at[1, s], fin_s.at[s], fin_r.at[s], across)

    def y_finish(t, es=every):
        for e in es:
            h, cb = place(t, e)
            ix = spot(t, e)

            def one():
                for d in range(2):
                    half, other = (U, T)[d], (T, U)[d]
                    arrived(ydst.at[ix, d, half], yo_s.at[d, ix], yo_r.at[d, ix])
                    arrived(ydst.at[ix, d, other], ya_s.at[d, ix], ya_r.at[d, ix])
                val = rounded(h, column(t, 0, e), red[ix, y] + ydst[ix, 0] + ydst[ix, 1])
                if moved(t) and e == 1:
                    fin[0, t % 3] = val
                    to_owner(t % 3).start()
                else:
                    c_ref[result(h, cb)] = val
            when(exists(t, 0, e), one)

    def from_opposite():
        for s in range(2):
            def one():
                arrived(fin.at[1, s], fin_s.at[s], fin_r.at[s])
                c_ref[result(2 * last + s, 1)] = fin[1, s]
            when(chips + x < 2 * last, one)

    def y_sent(t):
        for e in range(ents):
            ix = spot(t, e)
            for d in range(2):
                o, half, other = ahead[d], (U, T)[d], (T, U)[d]

                def sides():
                    left_us(red.at[ix, yy(o), half], yo_s.at[d, ix], yo_r.at[d, ix])
                    left_us(red.at[ix, yy(o), other], ya_s.at[d, ix], ya_r.at[d, ix])
                when(exists(t, 2, e), lambda: left_us(red.at[ix, yy(2), other], ym_s.at[d, ix], ym_r.at[d, ix]))
                when(exists(t, o, e), sides)

    zs = (items - 1) % slots
    pairs = [(g, e) for g in range(2) for e in range(2)]

    def z_exists(g, o):
        return yy(o) >= 2 * g + core

    def z_mid(g, e, d):
        return remote(part.at[zs, g, e, yy(2), (T, U)[d]], xmid.at[zs, d, e, g, T],
                      zm_s.at[d, g, e], zm_r.at[d, g, e], ydev[d])

    def z_side(g, e, d, half, s, r):
        return remote(part.at[zs, g, e, yy(ahead[d]), half], xdst.at[zs, d, e, g, half],
                      s.at[d, g, e], r.at[d, g, e], ydev[d])

    def z_own(g, e, d):
        return z_side(g, e, d, (U, T)[d], zo_s, zo_r)

    def z_acc(g, e, d):
        return z_side(g, e, d, (T, U)[d], za_s, za_r)

    def away(g):
        return lax.rem((2 * last + g) % chips + chips - x, chips)

    def w_mid(g, e, d):
        return remote(part.at[zs, g, e, y, (T, U)[d]], xmid.at[zs, d, e, 0, U], wm_s.at[d, e], wm_r.at[d, e], xdev[d])

    def w_side(g, e, d, half, s, r):
        return remote(part.at[zs, g, e, y, half], xdst.at[zs, d, e, 2, half], s.at[d, e], r.at[d, e], xdev[d])

    def w_own(g, e, d):
        return w_side(g, e, d, (U, T)[d], wo_s, wo_r)

    def w_acc(g, e, d):
        return w_side(g, e, d, (T, U)[d], wa_s, wa_r)

    def z_compute():
        x_sent(items - 1 - slots)

        def one(i, _):
            g, e = lax.div(i, 2), lax.rem(i, 2)
            part[zs, g, e] = product(last, e, 2 * last + g)
            return 0
        lax.fori_loop(0, 4, one, 0)
        take_credit(2)
        for g, e in pairs:
            when(z_exists(g, 2), lambda: [z_mid(g, e, d).start() for d in range(2)] and None)
        for g, e in pairs:
            for d in range(2):
                when(z_exists(g, ahead[d]), lambda: z_own(g, e, d).start())

    def z_pass_on():
        for g, e in pairs:
            for d in range(2):
                half = (T, U)[d]

                def one():
                    arrived(xmid.at[zs, d, e, g, T], zm_s.at[d, g, e], zm_r.at[d, g, e])
                    part[zs, g, e, yy(ahead[d]), half] += xmid[zs, d, e, g, T]
                    z_acc(g, e, d).start()
                when(z_exists(g, ahead[d]), one)

    def z_turn():
        take_credit(0)
        for g, e in pairs:
            def one():
                for d in range(2):
                    half, other = (U, T)[d], (T, U)[d]
                    arrived(xdst.at[zs, d, e, g, half], zo_s.at[d, g, e], zo_r.at[d, g, e])
                    arrived(xdst.at[zs, d, e, g, other], za_s.at[d, g, e], za_r.at[d, g, e])
                part[zs, g, e, y] = part[zs, g, e, y] + xdst[zs, 0, e, g] + xdst[zs, 1, e, g]
                pl.when(away(g) == 2)(lambda: [w_mid(g, e, d).start() for d in range(2)] and None)
                pl.when(away(g) == 1)(lambda: w_own(g, e, 0).start())
                pl.when(away(g) == chips - 1)(lambda: w_own(g, e, 1).start())
            when(z_exists(g, 0), one)

    def w_pass_on():
        for g, e in pairs:
            for d in range(2):
                half = (T, U)[d]

                def one():
                    arrived(xmid.at[zs, d, e, 0, U], wm_s.at[d, e], wm_r.at[d, e])
                    part[zs, g, e, y, half] += xmid[zs, d, e, 0, U]
                    w_acc(g, e, d).start()
                when(z_exists(g, 0) & (away(g) == (1, chips - 1)[d]), one)

    def w_finish():
        for g, e in pairs:
            def one():
                for d in range(2):
                    half, other = (U, T)[d], (T, U)[d]
                    arrived(xdst.at[zs, d, e, 2, half], wo_s.at[d, e], wo_r.at[d, e])
                    arrived(xdst.at[zs, d, e, 2, other], wa_s.at[d, e], wa_r.at[d, e])
                val = part[zs, g, e, y] + xdst[zs, 0, e, 2] + xdst[zs, 1, e, 2]
                m = 2 * last + g
                c_ref[result(2 * last + e, m // chips)] = rounded(2 * last + e, m, val)
            when(z_exists(g, 0) & (away(g) == 0), one)

    def z_sent():
        for g, e in pairs:
            for d in range(2):
                half, other = (U, T)[d], (T, U)[d]

                def sides():
                    left_us(part.at[zs, g, e, yy(ahead[d]), half], zo_s.at[d, g, e], zo_r.at[d, g, e])
                    left_us(part.at[zs, g, e, yy(ahead[d]), other], za_s.at[d, g, e], za_r.at[d, g, e])

                def w_sides():
                    left_us(part.at[zs, g, e, y, half], wo_s.at[d, e], wo_r.at[d, e])
                    left_us(part.at[zs, g, e, y, other], wa_s.at[d, e], wa_r.at[d, e])
                when(z_exists(g, 2), lambda: left_us(part.at[zs, g, e, yy(2), other], zm_s.at[d, g, e], zm_r.at[d, g, e]))
                when(z_exists(g, ahead[d]), sides)
                when(z_exists(g, 0) & (away(g) == 2),
                     lambda: left_us(part.at[zs, g, e, y, other], wm_s.at[d, e], wm_r.at[d, e]))
                when(z_exists(g, 0) & (away(g) == (1, chips - 1)[d]), w_sides)

    def half_of(t):
        return 2 * div(t, 3) + rem(t, 3)

    def have(t):
        h = half_of(t)
        own(h).wait()
        for d in range(2):
            arrived(x_piece(h, yy(rows - 1 if d == 0 else 1), 0, width), d_s.at[d, h], d_r.at[d, h])
            arrived(x_piece(h, yy(2), d * half_w, half_w), f_s.at[d, h], f_r.at[d, h])
        to_twin(h).start()

    def more(t):
        h = half_of(t)
        when(h + 1 < steps, lambda: pass_on(h + 1))

        def new():
            both(relay_out, h + 2)
            both(direct, h + 2)
        when(h + 2 < steps, new)

    def loop(lo, hi, f):
        def body(i, _):
            f(i)
            return 0
        lax.fori_loop(lo, hi, body, 0)

    both(relay_out, 0)
    both(direct, 0)
    loop(0, steps, lambda h: own(h).start())
    c_ref[...] = jnp.zeros_like(c_ref)
    pass_on(0)
    both(relay_out, 1)
    both(direct, 1)

    def step(t):
        when(rem(t, 3) < 2, lambda: have(t))
        compute(t)
        when(rem(t, 3) < 2, lambda: more(t))
        when(t >= 1, lambda: x_pass_on(t - 1))
        when(t >= 2, lambda: x_finish(t - 2))

    loop(0, START, step)

    acts = {"H": have, "G": more, "C": compute, "p": x_pass_on, "f": x_finish, "S": y_send, "P": y_pass_on,
            "F": y_finish, "Z": lambda n: (z_compute, z_pass_on, z_turn, w_pass_on, w_finish)[n]()}
    for act in TAIL:
        if act[-1] in "ab":
            acts[act[0]](int(act[1:-1]), ("ab".index(act[-1]),))
        else:
            acts[act[0]](int(act[1:]))
    from_opposite()

    def drain(h):
        for d in range(2):
            left_us(a_piece(h, yy(1), 0, width), d_s.at[d, h], d_r.at[d, h])
            left_us(a_piece(h, yy(2), 0, half_w), r_s.at[d, h], r_r.at[d, h])
            left_us(relay.at[d, h], f_s.at[d, h], f_r.at[d, h])
        left_us(twin_rows(h, 0), core_s.at[h], core_r.at[h])

    loop(0, steps, drain)
    z_sent()
    for t in range(items - slots, items - 1):
        x_sent(t)
    for s in range(2):
        when(chips + xx(2) < 2 * last, lambda: left_us(fin.at[0, s], fin_s.at[s], fin_r.at[s]))
    loop(0, items - 3, y_sent)
    for t in range(items - 3, items - 1):
        y_sent(t)


def solution(mesh):
    rows, cols = mesh.shape["row"], mesh.shape["col"]

    def local_fn(a_local):
        local_rows, m_local = a_local.shape
        steps, waves = local_rows // HALF, local_rows // BLOCK
        width = m_local // rows
        chips = cols // 2
        cbs = local_rows * rows // (BLOCK * cols)
        slots, spots = 3, steps + steps // 2
        dma = pltpu.SemaphoreType.DMA
        c, _ = pl.pallas_call(
            functools.partial(kernel, rows, cols),
            out_shape=(
                jax.ShapeDtypeStruct((local_rows, cbs * BLOCK), a_local.dtype),
                jax.ShapeDtypeStruct((2, steps, HALF, width // 2), a_local.dtype),
            ),
            in_specs=[pl.BlockSpec(memory_space=pltpu.HBM)],
            out_specs=(pl.BlockSpec(memory_space=pltpu.VMEM), pl.BlockSpec(memory_space=pltpu.HBM)),
            scratch_shapes=[
                pltpu.VMEM((waves, rows, BLOCK, 2 * width), a_local.dtype),
                pltpu.VMEM((slots, chips - 1, cbs, rows, HALF, BLOCK), F32),
                pltpu.VMEM((slots, 2, cbs, 2, HALF, BLOCK), F32),
                pltpu.VMEM((slots, 2, cbs, rows, HALF, BLOCK), F32),
                pltpu.VMEM((spots, rows, HALF, BLOCK), F32),
                pltpu.VMEM((spots, 2, QUART, BLOCK), F32),
                pltpu.VMEM((spots, 2, HALF, BLOCK), F32),
                pltpu.VMEM((2, 2, HALF, BLOCK), a_local.dtype),
            ] + [dma((2, steps))] * 6 + [dma((steps,))] * 3 + [dma((2, slots, cbs))] * 6 + [dma((2, spots))] * 6
            + [dma((2, 2, 2))] * 6 + [dma((2, 2))] * 6 + [dma((2,))] * 2 + [pltpu.SemaphoreType.REGULAR((4,))],
            compiler_params=pltpu.CompilerParams(
                collective_id=0, has_side_effects=True, vmem_limit_bytes=67043328),
        )(a_local)
        return c

    spec = P(("batch", "row"), "col")
    return jax.shard_map(local_fn, mesh=mesh, in_specs=(spec,), out_specs=spec, check_vma=False)
```

```python
import functools

import jax
import jax.numpy as jnp
from jax import lax
from jax.experimental import pallas as pl
from jax.experimental.pallas import tpu as pltpu
from jax.sharding import PartitionSpec as P

BLOCK = 256
HALF = BLOCK // 2
QUART = BLOCK // 4
MESH = pl.DeviceIdType.MESH
F32 = jnp.float32
START = 6
TAIL = (
    "p5", "H6", "G6", "C6", "f4", "H7", "f5", "p6", "C7", "G7", "f6", "C8", "H9", "S4", "p7", "C9", "f7",
    "S3", "G9", "p9b", "S6", "H10", "S7", "P6", "P3", "p8", "S2", "p9a", "C10", "P7", "f8", "S8", "P4", "P2",
    "Z0", "f9a", "Z1", "f9b", "S9a", "p10b", "S5", "P8", "P5", "S9b", "F6", "F2", "p10a", "P9a", "f10b",
    "S10b", "P10b", "F5", "Z2", "P9b", "f10a", "F8", "S10a", "F10b", "F9b", "Z3", "F7", "F9a", "P10a", "F3",
    "F10a", "Z4", "F4",
)


def kernel(rows, cols, a_ref, c_ref, relay, xin, part, xmid, xdst, red, ymid, ydst, fin,
           d_s, d_r, r_s, r_r, f_s, f_r, loc_s, core_s, core_r,
           xm_s, xm_r, xo_s, xo_r, xa_s, xa_r, ym_s, ym_r, yo_s, yo_r, ya_s, ya_r,
           zm_s, zm_r, zo_s, zo_r, za_s, za_r, wm_s, wm_r, wo_s, wo_r, wa_s, wa_r, fin_s, fin_r, credit):
    chips = cols // 2
    y = lax.axis_index("row")
    pos = lax.axis_index("col")
    x, core = lax.div(pos, 2), lax.rem(pos, 2)
    local_rows, m_local = a_ref.shape
    width = m_local // rows
    half_w = width // 2
    steps = local_rows // HALF
    items = 3 * steps // 2
    last = steps // 2 - 1
    late = steps - steps // 2
    slots, ents = part.shape[0], part.shape[2]
    every = tuple(range(ents))

    def div(p, q):
        return p // q if isinstance(p, int) else lax.div(p, q)

    def rem(p, q):
        return p % q if isinstance(p, int) else lax.rem(p, q)

    def when(test, f):
        if isinstance(test, bool):
            if test:
                f()
        else:
            pl.when(test)(f)

    def yy(o):
        return lax.rem(y + o, rows)

    def xx(o):
        return lax.rem(x + o, chips)

    up, down = {"row": yy(1)}, {"row": yy(rows - 1)}
    right, left = {"col": 2 * xx(1) + core}, {"col": 2 * xx(chips - 1) + core}
    across = {"col": 2 * xx(2) + core}
    twin = {"col": 2 * x + 1 - core}
    ydev, xdev = (up, down), (right, left)

    def remote(src, dst, s, r, dev):
        return pltpu.make_async_remote_copy(
            src_ref=src, dst_ref=dst, send_sem=s, recv_sem=r, device_id=dev, device_id_type=MESH)

    def arrived(dst, s, r):
        remote(dst, dst, s, r, twin).wait_recv()

    def left_us(src, s, r):
        remote(src, src, s, r, twin).wait_send()

    def signal(sem, dev):
        pl.semaphore_signal(sem, inc=1, device_id=dev, device_id_type=MESH)

    barrier = pltpu.get_barrier_semaphore()
    for dev in (up, down, right, left, across, twin):
        signal(barrier, dev)
    pl.semaphore_wait(barrier, 6)

    def half_rows(h):
        return pl.ds(pl.multiple_of(rem(h, 2) * HALF, HALF), HALF)

    def a_piece(h, owner, off, size):
        return a_ref.at[pl.ds(pl.multiple_of(h * HALF, HALF), HALF),
                        pl.ds(pl.multiple_of(owner * width + off, 128), size)]

    def x_piece(h, group, off, size):
        return xin.at[div(h, 2), group, half_rows(h), pl.ds(off, size)]

    def direct(h, d):
        return remote(a_piece(h, yy(1 if d == 0 else rows - 1), 0, width), x_piece(h, y, 0, width),
                      d_s.at[d, h], d_r.at[d, h], ydev[d])

    def relay_out(h, d):
        return remote(a_piece(h, yy(2), d * half_w, half_w), relay.at[d, h], r_s.at[d, h], r_r.at[d, h], ydev[d])

    def forward(h, d):
        return remote(relay.at[d, h], x_piece(h, yy(rows - 1 if d == 0 else 1), d * half_w, half_w),
                      f_s.at[d, h], f_r.at[d, h], ydev[d])

    def own(h):
        return pltpu.make_async_copy(a_piece(h, y, 0, width), x_piece(h, y, 0, width), loc_s.at[h])

    def twin_rows(h, off):
        return xin.at[div(h, 2), :, half_rows(h), pl.ds(off, width)]

    def to_twin(h):
        return remote(twin_rows(h, 0), twin_rows(h, width), core_s.at[h], core_r.at[h], twin)

    def both(f, h):
        for d in range(2):
            f(h, d).start()

    def pass_on(h):
        for d in range(2):
            arrived(relay.at[d, h], r_s.at[d, h], r_r.at[d, h])
        both(forward, h)

    def split(t):
        w, kind = div(t, 3), rem(t, 3)
        return w, kind, div(kind, 2)

    def choose(own_cols, before, inside):
        if isinstance(own_cols, int):
            return inside if own_cols else before
        return ((own_cols == 0) & before) | ((own_cols == 1) & inside)

    def place(t, e):
        w, kind, own_cols = split(t)
        return 2 * w + (1 - own_cols) * kind + own_cols * e, (1 - own_cols) * e + own_cols * div(2 * w, chips)

    def spot(t, e):
        h, cb = place(t, e)
        return h + late * cb

    def moved(t):
        return isinstance(t, int) and t // 3 == last and t % 3 < 2

    def column(t, o, e):
        return chips * place(t, e)[1] + xx(o + 2 * e if moved(t) else o)

    def low(t, o, e):
        w, _, own_cols = split(t)
        m = column(t, o, e)
        return choose(own_cols, m < 2 * w, m == 2 * w)

    def high(t, o, e):
        w, _, own_cols = split(t)
        m = column(t, o, e)
        return choose(own_cols, m < 2 * w, lax.div(m, 2) == w)

    A, B = pl.ds(0, 2), pl.ds(2, 2)

    def product(w, h, m):
        j = 2 * m + core
        lhs = xin[w, :, half_rows(h), :].reshape(rows * HALF, 2 * width)
        rhs = xin[lax.div(j, rows), lax.rem(j, rows)]
        val = lax.dot_general(lhs, rhs, (((1,), (1,)), ((), ())), preferred_element_type=F32)
        return val.reshape(rows, HALF, BLOCK)

    def x_mid(t, e, d):
        sl = rem(t, slots)
        return remote(part.at[sl, 1, e, (A, B)[d]], xmid.at[sl, d, e],
                      xm_s.at[d, sl, e], xm_r.at[d, sl, e], xdev[d])

    def x_own(t, e, d):
        sl, half = rem(t, slots), (B, A)[d]
        return remote(part.at[sl, 2 * d, e, half], xdst.at[sl, d, e, half],
                      xo_s.at[d, sl, e], xo_r.at[d, sl, e], xdev[d])

    def x_acc(t, e, d):
        sl, half = rem(t, slots), (A, B)[d]
        return remote(part.at[sl, 2 * d, e, half], xdst.at[sl, d, e, half],
                      xa_s.at[d, sl, e], xa_r.at[d, sl, e], xdev[d])

    def x_send_mid(t):
        for e in reversed(every) if moved(t) else every:
            when(low(t, 2, e), lambda: x_mid(t, e, 0).start())
            when(high(t, 2, e), lambda: x_mid(t, e, 1).start())

    def x_send_own(t, d):
        for e in reversed(every) if moved(t) else every:
            when(high(t, 1, e) if d == 0 else low(t, chips - 1, e), lambda: x_own(t, e, d).start())

    def x_pass_on(t, es=every):
        sl = rem(t, slots)
        for e in es:
            for d, o, half, test in ((0, 1, A, low), (1, chips - 1, B, high)):
                def one():
                    arrived(xmid.at[sl, d, e], xm_s.at[d, sl, e], xm_r.at[d, sl, e])
                    part[sl, 2 * d, e, half] += xmid[sl, d, e]
                    x_acc(t, e, d).start()
                when(test(t, o, e), one)

    def x_finish(t, es=every):
        sl = rem(t, slots)
        for e in es:
            ix = spot(t, e)

            def first():
                arrived(xdst.at[sl, 0, e, A], xa_s.at[0, sl, e], xa_r.at[0, sl, e])
                arrived(xdst.at[sl, 1, e, A], xo_s.at[1, sl, e], xo_r.at[1, sl, e])
                red[ix, A] = red[ix, A] + xdst[sl, 0, e, A] + xdst[sl, 1, e, A]

            def second():
                arrived(xdst.at[sl, 0, e, B], xo_s.at[0, sl, e], xo_r.at[0, sl, e])
                arrived(xdst.at[sl, 1, e, B], xa_s.at[1, sl, e], xa_r.at[1, sl, e])
                red[ix, B] = red[ix, B] + xdst[sl, 0, e, B] + xdst[sl, 1, e, B]
            when(low(t, 0, e), first)
            when(high(t, 0, e), second)
        if not isinstance(t, int) or t + slots < items:
            signal(credit.at[0], left)
            signal(credit.at[1], right)
        if isinstance(t, int) and t + slots == items - 1:
            signal(credit.at[2], up)
            signal(credit.at[3], down)

    def x_sent(t):
        sl = rem(t, slots)
        for e in range(ents):
            for o, d, half, s, r, test in (
                    (2, 0, A, xm_s, xm_r, low), (2, 1, B, xm_s, xm_r, high),
                    (1, 0, B, xo_s, xo_r, high), (chips - 1, 1, A, xo_s, xo_r, low),
                    (1, 0, A, xa_s, xa_r, low), (chips - 1, 1, B, xa_s, xa_r, high)):
                when(test(t, o, e), lambda: left_us(part.at[sl, o - 1, e, half], s.at[d, sl, e], r.at[d, sl, e]))

    def take_credit(first):
        pl.semaphore_wait(credit.at[first], 1)
        pl.semaphore_wait(credit.at[first + 1], 1)

    def compute(t):
        w, kind, _ = split(t)
        sl = rem(t, slots)

        def twin_in():
            h = 2 * w + kind
            arrived(twin_rows(h, width), core_s.at[h], core_r.at[h])
        when(kind < 2, twin_in)
        when(t >= slots, lambda: x_sent(t - slots))

        def one(i, _):
            n, e = lax.div(i, 2), 1 - lax.rem(i, 2) if moved(t) else lax.rem(i, 2)
            o = lax.rem(2 + 3 * n + 3 * lax.div(n, 2) + 2 * lax.div(n, 3), chips)
            m = column(t, o, e)

            @pl.when(high(t, o, e))
            def _():
                h, cb = place(t, e)
                val = product(w, h, m)

                @pl.when(o == 0)
                def _():
                    red[h + late * cb] = val

                @pl.when(o > 0)
                def _():
                    part[sl, o - 1, e] = val

            @pl.when(i == 1)
            def _():
                when(t >= slots, lambda: take_credit(0))
                x_send_mid(t)

            @pl.when(i == 3)
            def _():
                x_send_own(t, 0)

            @pl.when(i == 5)
            def _():
                x_send_own(t, 1)
            return 0

        lax.fori_loop(0, 2 * chips, one, 0)

    T, U = pl.ds(0, QUART), pl.ds(QUART, QUART)
    ahead = (1, rows - 1)

    def exists(t, o, e):
        w, _, own_cols = split(t)
        m = column(t, 0, e)
        return choose(own_cols, m < 2 * w, (lax.div(m, 2) == w) & (rows * w + yy(o) >= 2 * m + core))

    def y_mid(ix, d):
        return remote(red.at[ix, yy(2), (T, U)[d]], ymid.at[ix, d], ym_s.at[d, ix], ym_r.at[d, ix], ydev[d])

    def y_own(ix, d):
        half = (U, T)[d]
        return remote(red.at[ix, yy(ahead[d]), half], ydst.at[ix, d, half], yo_s.at[d, ix], yo_r.at[d, ix], ydev[d])

    def y_acc(ix, d):
        half = (T, U)[d]
        return remote(red.at[ix, yy(ahead[d]), half], ydst.at[ix, d, half], ya_s.at[d, ix], ya_r.at[d, ix], ydev[d])

    def y_send(t, es=every):
        for e in es:
            when(exists(t, 2, e), lambda: [y_mid(spot(t, e), d).start() for d in range(2)] and None)
        for e in es:
            for d in range(2):
                when(exists(t, ahead[d], e), lambda: y_own(spot(t, e), d).start())

    def y_pass_on(t, es=every):
        for e in es:
            ix = spot(t, e)
            for d in range(2):
                o, half = ahead[d], (T, U)[d]

                def one():
                    arrived(ymid.at[ix, d], ym_s.at[d, ix], ym_r.at[d, ix])
                    red[ix, yy(o), half] += ymid[ix, d]
                    y_acc(ix, d).start()
                when(exists(t, o, e), one)

    def rounded(h, m, val):
        i = (rows * div(h, 2) + y) * BLOCK + rem(h, 2) * HALF + lax.broadcasted_iota(jnp.int32, val.shape, 0)
        j = (2 * m + core) * BLOCK + lax.broadcasted_iota(jnp.int32, val.shape, 1)
        return jnp.where(i >= j, val, 0.0).astype(c_ref.dtype)

    def result(h, cb):
        return (pl.ds(pl.multiple_of(h * HALF, HALF), HALF), pl.ds(pl.multiple_of(cb * BLOCK, BLOCK), BLOCK))

    def to_owner(s):
        return remote(fin.at[0, s], fin.at[1, s], fin_s.at[s], fin_r.at[s], across)

    def y_finish(t, es=every):
        for e in es:
            h, cb = place(t, e)
            ix = spot(t, e)

            def one():
                for d in range(2):
                    half, other = (U, T)[d], (T, U)[d]
                    arrived(ydst.at[ix, d, half], yo_s.at[d, ix], yo_r.at[d, ix])
                    arrived(ydst.at[ix, d, other], ya_s.at[d, ix], ya_r.at[d, ix])
                val = rounded(h, column(t, 0, e), red[ix, y] + ydst[ix, 0] + ydst[ix, 1])
                if moved(t) and e == 1:
                    fin[0, t % 3] = val
                    to_owner(t % 3).start()
                else:
                    c_ref[result(h, cb)] = val
            when(exists(t, 0, e), one)

    def from_opposite():
        for s in range(2):
            def one():
                arrived(fin.at[1, s], fin_s.at[s], fin_r.at[s])
                c_ref[result(2 * last + s, 1)] = fin[1, s]
            when(chips + x < 2 * last, one)

    def y_sent(t):
        for e in range(ents):
            ix = spot(t, e)
            for d in range(2):
                o, half, other = ahead[d], (U, T)[d], (T, U)[d]

                def sides():
                    left_us(red.at[ix, yy(o), half], yo_s.at[d, ix], yo_r.at[d, ix])
                    left_us(red.at[ix, yy(o), other], ya_s.at[d, ix], ya_r.at[d, ix])
                when(exists(t, 2, e), lambda: left_us(red.at[ix, yy(2), other], ym_s.at[d, ix], ym_r.at[d, ix]))
                when(exists(t, o, e), sides)

    zs = (items - 1) % slots
    pairs = [(g, e) for g in range(2) for e in range(2)]

    def z_exists(g, o):
        return yy(o) >= 2 * g + core

    def z_mid(g, e, d):
        return remote(part.at[zs, g, e, yy(2), (T, U)[d]], xmid.at[zs, d, e, g, T],
                      zm_s.at[d, g, e], zm_r.at[d, g, e], ydev[d])

    def z_side(g, e, d, half, s, r):
        return remote(part.at[zs, g, e, yy(ahead[d]), half], xdst.at[zs, d, e, g, half],
                      s.at[d, g, e], r.at[d, g, e], ydev[d])

    def z_own(g, e, d):
        return z_side(g, e, d, (U, T)[d], zo_s, zo_r)

    def z_acc(g, e, d):
        return z_side(g, e, d, (T, U)[d], za_s, za_r)

    def away(g):
        return lax.rem((2 * last + g) % chips + chips - x, chips)

    def w_mid(g, e, d):
        return remote(part.at[zs, g, e, y, (T, U)[d]], xmid.at[zs, d, e, 0, U], wm_s.at[d, e], wm_r.at[d, e], xdev[d])

    def w_side(g, e, d, half, s, r):
        return remote(part.at[zs, g, e, y, half], xdst.at[zs, d, e, 2, half], s.at[d, e], r.at[d, e], xdev[d])

    def w_own(g, e, d):
        return w_side(g, e, d, (U, T)[d], wo_s, wo_r)

    def w_acc(g, e, d):
        return w_side(g, e, d, (T, U)[d], wa_s, wa_r)

    def z_compute():
        x_sent(items - 1 - slots)

        def one(i, _):
            g, e = lax.div(i, 2), lax.rem(i, 2)
            part[zs, g, e] = product(last, e, 2 * last + g)
            return 0
        lax.fori_loop(0, 4, one, 0)
        take_credit(2)
        for g, e in pairs:
            when(z_exists(g, 2), lambda: [z_mid(g, e, d).start() for d in range(2)] and None)
        for g, e in pairs:
            for d in range(2):
                when(z_exists(g, ahead[d]), lambda: z_own(g, e, d).start())

    def z_pass_on():
        for g, e in pairs:
            for d in range(2):
                half = (T, U)[d]

                def one():
                    arrived(xmid.at[zs, d, e, g, T], zm_s.at[d, g, e], zm_r.at[d, g, e])
                    part[zs, g, e, yy(ahead[d]), half] += xmid[zs, d, e, g, T]
                    z_acc(g, e, d).start()
                when(z_exists(g, ahead[d]), one)

    def z_turn():
        take_credit(0)
        for g, e in pairs:
            def one():
                for d in range(2):
                    half, other = (U, T)[d], (T, U)[d]
                    arrived(xdst.at[zs, d, e, g, half], zo_s.at[d, g, e], zo_r.at[d, g, e])
                    arrived(xdst.at[zs, d, e, g, other], za_s.at[d, g, e], za_r.at[d, g, e])
                part[zs, g, e, y] = part[zs, g, e, y] + xdst[zs, 0, e, g] + xdst[zs, 1, e, g]
                pl.when(away(g) == 2)(lambda: [w_mid(g, e, d).start() for d in range(2)] and None)
                pl.when(away(g) == 1)(lambda: w_own(g, e, 0).start())
                pl.when(away(g) == chips - 1)(lambda: w_own(g, e, 1).start())
            when(z_exists(g, 0), one)

    def w_pass_on():
        for g, e in pairs:
            for d in range(2):
                half = (T, U)[d]

                def one():
                    arrived(xmid.at[zs, d, e, 0, U], wm_s.at[d, e], wm_r.at[d, e])
                    part[zs, g, e, y, half] += xmid[zs, d, e, 0, U]
                    w_acc(g, e, d).start()
                when(z_exists(g, 0) & (away(g) == (1, chips - 1)[d]), one)

    def w_finish():
        for g, e in pairs:
            def one():
                for d in range(2):
                    half, other = (U, T)[d], (T, U)[d]
                    arrived(xdst.at[zs, d, e, 2, half], wo_s.at[d, e], wo_r.at[d, e])
                    arrived(xdst.at[zs, d, e, 2, other], wa_s.at[d, e], wa_r.at[d, e])
                val = part[zs, g, e, y] + xdst[zs, 0, e, 2] + xdst[zs, 1, e, 2]
                m = 2 * last + g
                c_ref[result(2 * last + e, m // chips)] = rounded(2 * last + e, m, val)
            when(z_exists(g, 0) & (away(g) == 0), one)

    def z_sent():
        for g, e in pairs:
            for d in range(2):
                half, other = (U, T)[d], (T, U)[d]

                def sides():
                    left_us(part.at[zs, g, e, yy(ahead[d]), half], zo_s.at[d, g, e], zo_r.at[d, g, e])
                    left_us(part.at[zs, g, e, yy(ahead[d]), other], za_s.at[d, g, e], za_r.at[d, g, e])

                def w_sides():
                    left_us(part.at[zs, g, e, y, half], wo_s.at[d, e], wo_r.at[d, e])
                    left_us(part.at[zs, g, e, y, other], wa_s.at[d, e], wa_r.at[d, e])
                when(z_exists(g, 2), lambda: left_us(part.at[zs, g, e, yy(2), other], zm_s.at[d, g, e], zm_r.at[d, g, e]))
                when(z_exists(g, ahead[d]), sides)
                when(z_exists(g, 0) & (away(g) == 2),
                     lambda: left_us(part.at[zs, g, e, y, other], wm_s.at[d, e], wm_r.at[d, e]))
                when(z_exists(g, 0) & (away(g) == (1, chips - 1)[d]), w_sides)

    def half_of(t):
        return 2 * div(t, 3) + rem(t, 3)

    def have(t):
        h = half_of(t)
        own(h).wait()
        for d in range(2):
            arrived(x_piece(h, yy(rows - 1 if d == 0 else 1), 0, width), d_s.at[d, h], d_r.at[d, h])
            arrived(x_piece(h, yy(2), d * half_w, half_w), f_s.at[d, h], f_r.at[d, h])
        to_twin(h).start()

    def more(t):
        h = half_of(t)
        when(h + 1 < steps, lambda: pass_on(h + 1))

        def new():
            both(relay_out, h + 2)
            both(direct, h + 2)
        when(h + 2 < steps, new)

    def loop(lo, hi, f):
        def body(i, _):
            f(i)
            return 0
        lax.fori_loop(lo, hi, body, 0)

    both(relay_out, 0)
    both(direct, 0)
    loop(0, steps, lambda h: own(h).start())
    c_ref[...] = jnp.zeros_like(c_ref)
    pass_on(0)
    both(relay_out, 1)
    both(direct, 1)

    def step(t):
        when(rem(t, 3) < 2, lambda: have(t))
        compute(t)
        when(rem(t, 3) < 2, lambda: more(t))
        when(t >= 1, lambda: x_pass_on(t - 1))
        when(t >= 2, lambda: x_finish(t - 2))

    loop(0, START, step)

    acts = {"H": have, "G": more, "C": compute, "p": x_pass_on, "f": x_finish, "S": y_send, "P": y_pass_on,
            "F": y_finish, "Z": lambda n: (z_compute, z_pass_on, z_turn, w_pass_on, w_finish)[n]()}
    for act in TAIL:
        if act[-1] in "ab":
            acts[act[0]](int(act[1:-1]), ("ab".index(act[-1]),))
        else:
            acts[act[0]](int(act[1:]))
    from_opposite()

    def drain(h):
        for d in range(2):
            left_us(a_piece(h, yy(1), 0, width), d_s.at[d, h], d_r.at[d, h])
            left_us(a_piece(h, yy(2), 0, half_w), r_s.at[d, h], r_r.at[d, h])
            left_us(relay.at[d, h], f_s.at[d, h], f_r.at[d, h])
        left_us(twin_rows(h, 0), core_s.at[h], core_r.at[h])

    loop(0, steps, drain)
    z_sent()
    for t in range(items - slots, items - 1):
        x_sent(t)
    for s in range(2):
        when(chips + xx(2) < 2 * last, lambda: left_us(fin.at[0, s], fin_s.at[s], fin_r.at[s]))
    loop(0, items - 3, y_sent)
    for t in range(items - 3, items - 1):
        y_sent(t)


def solution(mesh):
    rows, cols = mesh.shape["row"], mesh.shape["col"]

    def local_fn(a_local):
        local_rows, m_local = a_local.shape
        steps, waves = local_rows // HALF, local_rows // BLOCK
        width = m_local // rows
        chips = cols // 2
        cbs = local_rows * rows // (BLOCK * cols)
        slots, spots = 3, steps + steps // 2
        dma = pltpu.SemaphoreType.DMA
        c, _ = pl.pallas_call(
            functools.partial(kernel, rows, cols),
            out_shape=(
                jax.ShapeDtypeStruct((local_rows, cbs * BLOCK), a_local.dtype),
                jax.ShapeDtypeStruct((2, steps, HALF, width // 2), a_local.dtype),
            ),
            in_specs=[pl.BlockSpec(memory_space=pltpu.HBM)],
            out_specs=(pl.BlockSpec(memory_space=pltpu.VMEM), pl.BlockSpec(memory_space=pltpu.HBM)),
            scratch_shapes=[
                pltpu.VMEM((waves, rows, BLOCK, 2 * width), a_local.dtype),
                pltpu.VMEM((slots, chips - 1, cbs, rows, HALF, BLOCK), F32),
                pltpu.VMEM((slots, 2, cbs, 2, HALF, BLOCK), F32),
                pltpu.VMEM((slots, 2, cbs, rows, HALF, BLOCK), F32),
                pltpu.VMEM((spots, rows, HALF, BLOCK), F32),
                pltpu.VMEM((spots, 2, QUART, BLOCK), F32),
                pltpu.VMEM((spots, 2, HALF, BLOCK), F32),
                pltpu.VMEM((2, 2, HALF, BLOCK), a_local.dtype),
            ] + [dma((2, steps))] * 6 + [dma((steps,))] * 3 + [dma((2, slots, cbs))] * 6 + [dma((2, spots))] * 6
            + [dma((2, 2, 2))] * 6 + [dma((2, 2))] * 6 + [dma((2,))] * 2 + [pltpu.SemaphoreType.REGULAR((4,))],
            compiler_params=pltpu.CompilerParams(
                collective_id=0, has_side_effects=True, vmem_limit_bytes=67043328),
        )(a_local)
        return c

    spec = P(("batch", "row"), "col")
    return jax.shard_map(local_fn, mesh=mesh, in_specs=(spec,), out_specs=spec, check_vma=False)
```
